32 devices in a mesh: ens: 2 (over y), space: 4 (over z), chan: 2 (over x), sub: 2 (over core).
Axes of the slice: x: 2, y: 2, z: 4, core: 2. Of those that a mesh axis runs over, the one named last changes fastest.
Arguments:
- node_state: bfloat16 [8192, 512], P(('ens', 'space'), ('chan', 'sub')), parts along dimension 0, may hold values from -6 to 6
- norm_gains: float32 [2, 512], replicated, may hold values from 0.25 to 1.75
- norm_shifts: float32 [2, 512], replicated, may hold values from -3 to 3
- query_weight: bfloat16 [512, 512], P(None, 'chan')
- key_weight: bfloat16 [512, 512], P(None, 'chan')
- value_weight: bfloat16 [512, 512], P(None, 'chan'), may hold values from -0.25 to 0.25
- out_weight: bfloat16 [512, 512], replicated, may hold values from -0.25 to 0.25
- ffn_in: bfloat16 [2048, 512], P('chan'), may hold values from -0.25 to 0.25
- ffn_out: bfloat16 [2048, 512], P('chan'), may hold values from -0.125 to 0.125
- live_counts: int32 [4], P('space'), may hold values from 512 to 1024, as said below
- send_rows: int32 [4, 2, 256], P('space'), may hold values from 0 to 1023, as said below
- tile_keys: int32 [32, 12], P('space'), may hold values from 0 to 11, as said below
- tile_bits: int32 [32, 12, 4, 128], P('space'), may hold values from -2147483648 to 2147483647, as said below
Outputs:
- updated: bfloat16 [8192, 512], P(('ens', 'space'), ('chan', 'sub')), parts along dimension 0
The draws below stay inside these ranges and needn't reach their ends.
There are 2 independent parts, one for each index of `ens`. The reference program is written for one: setup_inputs(seed, part) draws one part's arguments, and reference() takes and returns one part's arrays. A program takes and returns all parts, laid end to end along the dimension named above; an argument that names none is the same for every part. Nothing has to cross between parts.
Inputs may be any that keep to these rules, and one draw needn't show every extreme that they name: Partition s has live nodes 0 to live_counts[s] - 1; the first and the last partition are full. send_rows[s, 0] lists nodes of partition s read by its lower neighbour, send_rows[s, 1] those read by its upper neighbour; all are live nodes, and entries may repeat. `tile_keys`: slot 0 of every block names the block itself (its index within the partition); other slots name blocks of the same partition (below 8), of the lower halo (from 8) or of the upper halo (from 10); the first partition names no lower halo and the last no upper halo. `tile_bits`: bit j of word w in column r of a slot says whether query r of the block may attend key 32 w + j of the slot's block (bit 31 is the sign bit); in slot 0 every query's own bit is set. Slots whose words are all zero carry no edges.
All inputs are finite; a program needn't handle non-finite values.
Results may differ from the reference program's by a relative error of at most 0.0095.
Values may be sent and summed in bfloat16 or wider, within the bound.
No kernel may reach another device: no remote copies, remote signals or barrier semaphores. Data moves between devices by JAX's collectives and lax.ppermute only.
A program may use at most 64 MiB of HBM per device.

```python
import math
import jax
import jax.numpy as jnp
from jax import lax

D = 512
HEADS = 8
HD = 64
FF = 2048
TILE = 128
WORDS = 4
KT = 12
HBLK = 2
HB = 256
NB = 8
NBK = 12
NODE_PART = 1024
NODES = 4096
BLOCKS = 32
N_SPACE = 4


def paired_projection(key):
    shared_part = jax.random.normal(jax.random.fold_in(key, 11), (D, D), jnp.float32) / math.sqrt(D)
    second_part = jax.random.normal(jax.random.fold_in(key, 12), (D, D), jnp.float32) / math.sqrt(D)
    return (shared_part, second_part)


def draw_query_weight(key, part):
    shared_part, second_part = paired_projection(key)
    return shared_part.astype(jnp.bfloat16)


def draw_key_weight(key, part):
    shared_part, second_part = paired_projection(key)
    return second_part.astype(jnp.bfloat16)


def partition_sizes(key):
    parts_total = BLOCKS // NB
    section = jnp.arange(parts_total, dtype=jnp.int32)
    drawn = jax.random.randint(jax.random.fold_in(key, 51), (parts_total,), NODE_PART // 2, NODE_PART + 1, dtype=jnp.int32)
    polar = (section == 0) | (section == parts_total - 1)
    return jnp.where(polar, NODE_PART, drawn)


def draw_live_counts(key, part):
    return partition_sizes(key)


def draw_send_rows(key, part):
    sizes = partition_sizes(key)
    return jax.random.randint(jax.random.fold_in(key, 61), (BLOCKS // NB, 2, HB), 0, sizes[:, None, None], dtype=jnp.int32)


def slot_use(key):
    blocks = jnp.arange(BLOCKS, dtype=jnp.int32)
    section = blocks // NB
    polar = (section == 0) | (section == BLOCKS // NB - 1)
    partial_use = jax.random.randint(jax.random.fold_in(key, 21), (BLOCKS,), (KT + 1) // 2, KT + 1, dtype=jnp.int32)
    return jnp.where(polar, KT, partial_use)


def draw_tile_keys(key, part):
    blocks = jnp.arange(BLOCKS, dtype=jnp.int32)
    local_block = blocks % NB
    section = blocks // NB
    offsets = jax.random.randint(jax.random.fold_in(key, 31), (BLOCKS, KT), 1, NB, dtype=jnp.int32)
    others = (local_block[:, None] + offsets) % NB
    near_low = local_block < NB // 2
    low_pick = NB + jax.random.randint(jax.random.fold_in(key, 32), (BLOCKS,), 0, HBLK, dtype=jnp.int32)
    high_pick = NB + HBLK + jax.random.randint(jax.random.fold_in(key, 33), (BLOCKS,), 0, HBLK, dtype=jnp.int32)
    halo_pick = jnp.where(near_low, low_pick, high_pick)
    outer_side = (section == 0) & near_low | (section == BLOCKS // NB - 1) & jnp.logical_not(near_low)
    second_slot = jnp.where(outer_side, others[:, 1], halo_pick)
    return jnp.concatenate([local_block[:, None], second_slot[:, None], others[:, 2:]], axis=1)


def draw_tile_bits(key, part):
    random_words = jax.random.randint(jax.random.fold_in(key, 41), (BLOCKS, KT, WORDS, TILE), -2147483647, 2147483647, dtype=jnp.int32)
    slot_live = (jnp.arange(KT, dtype=jnp.int32)[None, :] < slot_use(key)[:, None]).astype(jnp.int32)
    random_words = random_words * slot_live[:, :, None, None]
    rows_at = jnp.arange(TILE, dtype=jnp.int32)
    own_word = jnp.arange(WORDS, dtype=jnp.int32)[:, None] == (rows_at // 32)[None, :]
    diagonal = jnp.where(own_word, jnp.left_shift(jnp.int32(1), rows_at % 32)[None, :], jnp.int32(0))
    first_slot = jnp.bitwise_or(random_words[:, :1], diagonal[None, None])
    return jnp.concatenate([first_slot, random_words[:, 1:]], axis=1)


def block_levels(key, dims, cuts, smallest, top_value):
    factor_of = 1.0
    for dim, shards_of in cuts:
        draws = jax.random.uniform(jax.random.fold_in(jax.random.fold_in(key, 6), dim), (shards_of,), jnp.float32, smallest / len(cuts), top_value / len(cuts))
        factor_of = factor_of * jnp.repeat(jnp.exp(draws), dims[dim] // shards_of).reshape((-1,) + (1,) * (len(dims) - 1 - dim))
    return factor_of


def bell_draw(rng, shape, width, bound, shards=(), kind=jnp.bfloat16):
    values = jax.random.normal(rng, shape, jnp.float32) * width
    if len(shards) > 0:
        values = block_levels(rng, shape, shards, -0.22, 0.18) * values
    return jnp.clip(values, min=-bound, max=bound).astype(kind)


def setup_inputs(seed: int = 0, part: int = 0) -> dict:
    streams_of = jax.random.split(jax.random.key(seed), 14)
    own_keys = jax.random.split(jax.random.fold_in(streams_of[13], part), 14)
    return {
        "node_state": bell_draw(own_keys[0], (NODES, D), 1.0, 6.0, ((0, 4), (1, 4))),
        "norm_gains": jnp.clip(1.0 + 0.15 * jax.random.normal(streams_of[1], (2, D), jnp.float32), 0.25, 1.75),
        "norm_shifts": bell_draw(streams_of[2], (2, D), 0.5, 3.0, (), jnp.float32),
        "query_weight": draw_query_weight(jax.random.fold_in(streams_of[13], 71), part),
        "key_weight": draw_key_weight(jax.random.fold_in(streams_of[13], 71), part),
        "value_weight": bell_draw(streams_of[5], (D, D), D ** -0.5, 0.25, ((1, 2),)),
        "out_weight": bell_draw(streams_of[6], (D, D), D ** -0.5, 0.25),
        "ffn_in": bell_draw(streams_of[7], (FF, D), D ** -0.5, 0.25, ((0, 2),)),
        "ffn_out": bell_draw(streams_of[8], (FF, D), FF ** -0.5, 0.125, ((0, 2),)),
        "live_counts": draw_live_counts(jax.random.fold_in(streams_of[13], 71), part),
        "send_rows": draw_send_rows(jax.random.fold_in(streams_of[13], 71), part),
        "tile_keys": draw_tile_keys(jax.random.fold_in(streams_of[13], 71), part),
        "tile_bits": draw_tile_bits(jax.random.fold_in(streams_of[13], 71), part),
    }


NORM_EPS = 1e-05
NEG_FILL = -1e+30

def normalize_rows(source, gain_row, shift_row):
    row_mean = lax.optimization_barrier(jnp.mean(source, axis=-1, keepdims=True))
    spread = lax.optimization_barrier(jnp.mean(source * source, axis=-1, keepdims=True)) - row_mean * row_mean
    return (source - row_mean) * lax.rsqrt(spread + NORM_EPS) * gain_row + shift_row

def unpack_allowed(key_bits, key_ids, live_count, tile_size, blocks_own):
    shifts = jnp.arange(32, dtype=jnp.int32)
    expanded = jnp.right_shift(key_bits[..., None, :], shifts[:, None]) & 1
    lead_shape = key_bits.shape[:-2]
    expanded = expanded.reshape(lead_shape + (tile_size, tile_size))
    key_index = key_ids[..., None] * tile_size + jnp.arange(tile_size, dtype=jnp.int32)
    key_live = (key_ids[..., None] >= blocks_own) | (key_index < live_count)
    slot_count = key_ids.shape[-1]
    slot_first = jnp.arange(slot_count, dtype=jnp.int32)[:, None, None] == 0
    diagonal = jnp.arange(tile_size, dtype=jnp.int32)[:, None] == jnp.arange(tile_size, dtype=jnp.int32)[None, :]
    own_bit = slot_first & diagonal[None]
    return (expanded == 1) & (key_live[..., None] | own_bit)

def reference(node_state, norm_gains, norm_shifts, query_weight, key_weight, value_weight, out_weight, ffn_in, ffn_out, live_counts, send_rows, tile_keys, tile_bits):
    float_state = node_state.astype(jnp.float32)
    normed = normalize_rows(float_state, norm_gains[0], norm_shifts[0]).astype(jnp.bfloat16)
    queries = jnp.dot(normed, query_weight, preferred_element_type=jnp.float32).astype(jnp.bfloat16)
    key_rows = jnp.dot(normed, key_weight, preferred_element_type=jnp.float32).astype(jnp.bfloat16)
    value_rows = jnp.dot(normed, value_weight, preferred_element_type=jnp.float32).astype(jnp.bfloat16)
    key_values = jnp.concatenate([key_rows, value_rows], axis=1).reshape(N_SPACE, NODE_PART, 2 * D)
    upward = jnp.take_along_axis(key_values, send_rows[:, 1, :, None], axis=1)
    downward = jnp.take_along_axis(key_values, send_rows[:, 0, :, None], axis=1)
    empty_rim = jnp.zeros((1, HB, 2 * D), key_values.dtype)
    lower_rim = jnp.concatenate([empty_rim, upward[:-1]], axis=0)
    upper_rim = jnp.concatenate([downward[1:], empty_rim], axis=0)
    extended = jnp.concatenate([key_values, lower_rim, upper_rim], axis=1).reshape(N_SPACE, NBK, TILE, 2 * D)
    query_blocks = queries.reshape(N_SPACE, NB, TILE, HEADS, HD)
    key_ids = tile_keys.reshape(N_SPACE, NB, KT)
    key_bits = tile_bits.reshape(N_SPACE, NB, KT, WORDS, TILE)
    score_scale = 1.0 / math.sqrt(HD)

    def one_partition(inputs):
        ext_part, q_part, id_part, bit_part, count_part = inputs
        chosen = ext_part[id_part]
        keys_part = chosen[..., :D].reshape(NB, KT, TILE, HEADS, HD).astype(jnp.float32)
        values_part = chosen[..., D:].reshape(NB, KT, TILE, HEADS, HD).astype(jnp.float32)
        scores = jnp.einsum('brhd,btkhd->bhrtk', q_part.astype(jnp.float32), keys_part) * score_scale
        allowed = unpack_allowed(bit_part, id_part, count_part, TILE, NB)
        allowed = jnp.transpose(allowed, (0, 3, 1, 2))[:, None]
        masked = jnp.where(allowed, scores, NEG_FILL)
        row_max = lax.optimization_barrier(jnp.max(masked, axis=(3, 4), keepdims=True))
        weights = jnp.where(allowed, jnp.exp(scores - row_max), 0.0)
        row_total = lax.optimization_barrier(jnp.sum(weights, axis=(3, 4)))
        rounded = lax.optimization_barrier(weights.astype(jnp.bfloat16)).astype(jnp.float32)
        mixed_heads = jnp.einsum('bhrtk,btkhd->brhd', rounded, values_part)
        mixed_heads = mixed_heads / jnp.transpose(row_total, (0, 2, 1))[..., None]
        return mixed_heads.astype(jnp.bfloat16).reshape(NB * TILE, D)
    attended = lax.map(one_partition, (extended, query_blocks, key_ids, key_bits, live_counts)).reshape(NODES, D)
    after_attn = float_state + jnp.dot(attended, out_weight, preferred_element_type=jnp.float32)
    normed_two = normalize_rows(after_attn, norm_gains[1], norm_shifts[1]).astype(jnp.bfloat16)
    hidden = jax.nn.gelu(jnp.dot(normed_two, ffn_in.T, preferred_element_type=jnp.float32)).astype(jnp.bfloat16)
    result = after_attn + jnp.dot(hidden, ffn_out, preferred_element_type=jnp.float32)
    node_at = jnp.arange(NODES, dtype=jnp.int32)
    node_live = node_at % NODE_PART < live_counts[node_at // NODE_PART]
    return jnp.where(node_live[:, None], result, 0.0).astype(jnp.bfloat16)
```

```python
import functools
import math

import jax
import jax.numpy as jnp
from jax import lax
from jax.experimental import pallas as pl
from jax.experimental.pallas import tpu as pltpu
from jax.sharding import PartitionSpec as P

HD = 64


NORM_EPS = 1e-05
F32 = jnp.float32
BF16 = jnp.bfloat16
NT = (((1,), (1,)), ((), ()))
NN = (((1,), (0,)), ((), ()))


def dot(a, b, dims=NN):
    return lax.dot_general(a, b, dims, preferred_element_type=F32)


def normalize_rows(source, gain_row, shift_row):
    row_mean = jnp.mean(source, axis=-1, keepdims=True)
    spread = jnp.mean(source * source, axis=-1, keepdims=True) - row_mean * row_mean
    return (source - row_mean) * lax.rsqrt(spread + NORM_EPS) * gain_row + shift_row


def pick_body(list_ref, x_ref, up_ref, down_ref):
    rows = x_ref.shape[0]
    width = list_ref.shape[-1]
    source = x_ref[...]
    node = lax.broadcasted_iota(jnp.int32, (rows, width), 0)
    for at, out in ((1, up_ref), (0, down_ref)):
        hot = (node == list_ref[at : at + 1, :]).astype(F32).astype(BF16)
        out[...] = lax.dot_general(
            hot, source, (((0,), (0,)), ((), ())), preferred_element_type=F32
        ).astype(BF16)


def pick_rows(send_list, source):
    shape = jax.ShapeDtypeStruct((send_list.shape[1], source.shape[1]), source.dtype)
    return pl.pallas_call(pick_body, out_shape=(shape, shape), name="pick_rows")(send_list, source)


def project_body(chunk, pieces, meta_ref, *refs):
    mains, halos = refs[:pieces], refs[pieces : 2 * pieces]
    gain_ref, shift_ref, wq_ref, wk_ref, wvt_ref = refs[2 * pieces : 2 * pieces + 5]
    q_ref, k_ref, vt_ref, own_ref, xs_ref, ns_ref = refs[2 * pieces + 5 :]
    chan_at, sub_at = meta_ref[0], meta_ref[1]
    rows = mains[0].shape[0]
    cols = mains[0].shape[1]
    total = xs_ref.shape[0]
    for i in range(pieces):
        if pieces == 1:
            place = slice(None)
        else:
            chan_of = chan_at if i < 2 else 1 - chan_at
            sub_of = sub_at if i % 2 == 0 else 1 - sub_at
            place = pl.ds(pl.multiple_of((chan_of * 2 + sub_of) * cols, cols), cols)
        xs_ref[:rows, place] = mains[i][...]
        xs_ref[rows:, place] = halos[i][...]
    gain, shift = gain_ref[0:1, :], shift_ref[0:1, :]

    def step(j, carry):
        at = pl.ds(pl.multiple_of(j * chunk, chunk), chunk)
        normed = normalize_rows(xs_ref[at, :].astype(F32), gain, shift).astype(BF16)
        ns_ref[at, :] = normed
        k_ref[at, :] = dot(normed, wk_ref[...]).astype(BF16)
        vt_ref[:, at] = dot(wvt_ref[...], normed, NT).astype(BF16)
        return carry

    lax.fori_loop(0, total // chunk, step, 0)
    here = q_ref.shape[0]
    own = pl.ds(pl.multiple_of(sub_at * here, here), here)
    own_ref[...] = xs_ref[own, :]
    scale = 1.0 / math.sqrt(HD)
    q_ref[...] = (dot(ns_ref[own, :], wq_ref[...]).astype(BF16).astype(F32) * scale).astype(BF16)


def project(meta, mains, halos, gains, shifts, wq, wk, wvt, here):
    pieces = len(mains)
    total = mains[0].shape[0] + halos[0].shape[0]
    width = gains.shape[1]
    head_cols = wq.shape[1]
    vmem = pl.BlockSpec(memory_space=pltpu.VMEM)
    smem = pl.BlockSpec(memory_space=pltpu.SMEM)
    return pl.pallas_call(
        functools.partial(project_body, math.gcd(total, 256), pieces),
        out_shape=(
            jax.ShapeDtypeStruct((here, head_cols), BF16),
            jax.ShapeDtypeStruct((total, head_cols), BF16),
            jax.ShapeDtypeStruct((head_cols, total), BF16),
            jax.ShapeDtypeStruct((here, width), BF16),
        ),
        in_specs=[smem] + [vmem] * (2 * pieces + 5),
        out_specs=(vmem,) * 4,
        scratch_shapes=[pltpu.VMEM((total, width), BF16), pltpu.VMEM((total, width), BF16)],
        name="project",
    )(meta, *mains, *halos, gains, shifts, wq, wk, wvt)


def attend_body(
    blocks_own, meta_ref, live_ref, id_ref, q_ref, bit_ref, k_ref, vt_ref, out_ref, s_ref
):
    slot_count, word_count, tile = bit_ref.shape[1:]
    head_cols = q_ref.shape[1]
    heads = head_cols // HD
    block = meta_ref[1] * pl.num_programs(0) + pl.program_id(0)
    live = live_ref[0]
    q = q_ref[...]
    lane = lax.broadcasted_iota(jnp.int32, (tile, head_cols), 1)
    spread = jnp.concatenate(
        [jnp.where(lane // HD == h, q, jnp.zeros_like(q)) for h in range(heads)], axis=0
    )
    key_at = lax.broadcasted_iota(jnp.int32, (tile, tile), 0)
    query_at = lax.broadcasted_iota(jnp.int32, (tile, tile), 1)
    per_word = tile // word_count
    bit_at = lax.broadcasted_iota(jnp.int32, (per_word, tile), 0)
    peak = None
    starts = []
    for t in range(slot_count):
        key_id = id_ref[block, t]
        start = pl.multiple_of(key_id * tile, tile)
        starts.append(start)
        scores = dot(k_ref[pl.ds(start, tile), :], spread, NT)
        limit = jnp.where(key_id >= blocks_own, tile, live - key_id * tile)
        usable = key_at < limit
        if t == 0:
            usable = usable | (key_at == query_at)
        words = jnp.concatenate(
            [
                jnp.right_shift(
                    jnp.broadcast_to(bit_ref[0, t, w : w + 1, :], (per_word, tile)), bit_at
                )
                & 1
                for w in range(word_count)
            ],
            axis=0,
        )
        allowed = (words == 1) & usable
        for h in range(heads):
            part = jnp.where(allowed, scores[:, h * tile : (h + 1) * tile], -jnp.inf)
            s_ref[t * tile : (t + 1) * tile, h * tile : (h + 1) * tile] = part
        top = jnp.max(
            s_ref[t * tile : (t + 1) * tile, :].reshape(tile // 8, 8, heads * tile), axis=0
        )
        peak = top if peak is None else jnp.maximum(peak, top)
    peak = jnp.max(peak, axis=0, keepdims=True)
    group = math.gcd(heads, 2)
    per_dot = math.gcd(slot_count, 2)
    mixed = [None] * (heads // group)
    total = None
    for t in range(0, slot_count, per_dot):
        weights = jnp.exp(s_ref[t * tile : (t + per_dot) * tile, :] - peak)
        part = jnp.sum(weights.reshape(per_dot * tile // 8, 8, heads * tile), axis=0)
        total = part if total is None else total + part
        weights = weights.astype(BF16)
        for g in range(heads // group):
            values = jnp.concatenate(
                [
                    vt_ref[g * group * HD : (g + 1) * group * HD, pl.ds(starts[t + i], tile)]
                    for i in range(per_dot)
                ],
                axis=1,
            )
            add = dot(values, weights[:, g * group * tile : (g + 1) * group * tile])
            mixed[g] = add if mixed[g] is None else mixed[g] + add
    total = jnp.sum(total, axis=0, keepdims=True)
    pieces = []
    for h in range(heads):
        g, i = divmod(h, group)
        own = mixed[g][i * HD : (i + 1) * HD, i * tile : (i + 1) * tile]
        pieces.append(own / total[:, h * tile : (h + 1) * tile])
    out_ref[...] = jnp.concatenate(pieces, axis=0).T.astype(BF16)


def attend(meta, live_counts, tile_keys, queries, tile_bits, keys, values_t):
    blocks_own, slot_count, word_count, tile = tile_bits.shape
    here, head_cols = queries.shape
    total = keys.shape[0]
    count = here // tile
    heads = head_cols // HD
    return pl.pallas_call(
        functools.partial(attend_body, blocks_own),
        out_shape=jax.ShapeDtypeStruct((here, head_cols), BF16),
        grid_spec=pltpu.PrefetchScalarGridSpec(
            num_scalar_prefetch=3,
            grid=(count,),
            in_specs=[
                pl.BlockSpec((tile, head_cols), lambda i, m, n, k: (i, 0)),
                pl.BlockSpec(
                    (1, slot_count, word_count, tile),
                    lambda i, m, n, k: (m[1] * count + i, 0, 0, 0),
                ),
                pl.BlockSpec((total, head_cols), lambda i, m, n, k: (0, 0)),
                pl.BlockSpec((head_cols, total), lambda i, m, n, k: (0, 0)),
            ],
            out_specs=pl.BlockSpec((tile, head_cols), lambda i, m, n, k: (i, 0)),
            scratch_shapes=[pltpu.VMEM((slot_count * tile, heads * tile), F32)],
        ),
        name="attend",
    )(meta, live_counts, tile_keys, queries, tile_bits, keys, values_t)


def feed_body(chunk, paired, meta_ref, *refs):
    count = 2 if paired else 1
    mixed = refs[:count]
    x_ref, wo_ref, gain_ref, shift_ref, in_ref, out_w_ref, send_ref, keep_ref = refs[count:]
    chan_at = meta_ref[0]
    here, width = x_ref.shape
    gain, shift = gain_ref[1:2, :], shift_ref[1:2, :]

    def step(j, carry):
        at = pl.ds(pl.multiple_of(j * chunk, chunk), chunk)
        after = x_ref[at, :].astype(F32)
        for i in range(count):
            cols = mixed[i].shape[1]
            if paired:
                chan_of = chan_at if i == 0 else 1 - chan_at
                weight = wo_ref[pl.ds(pl.multiple_of(chan_of * cols, cols), cols), :]
            else:
                weight = wo_ref[...]
            after = after + dot(mixed[i][at, :], weight)
        normed = normalize_rows(after, gain, shift).astype(BF16)
        hidden = jax.nn.gelu(dot(normed, in_ref[...], NT)).astype(BF16)
        update = dot(hidden, out_w_ref[...])
        if paired:
            half = width // 2
            first = chan_at == 0
            send_ref[at, :] = jnp.where(first, update[:, half:], update[:, :half]).astype(BF16)
            both = after + update
            keep_ref[at, :] = jnp.where(first, both[:, :half], both[:, half:])
        else:
            send_ref[at, :] = update.astype(BF16)
            keep_ref[at, :] = after
        return carry

    lax.fori_loop(0, here // chunk, step, 0)


def feed(meta, mixed, own_x, out_weight, gains, shifts, ffn_in, ffn_out):
    paired = len(mixed) == 2
    here, width = own_x.shape
    cols = width // 2 if paired else width
    vmem = pl.BlockSpec(memory_space=pltpu.VMEM)
    smem = pl.BlockSpec(memory_space=pltpu.SMEM)
    return pl.pallas_call(
        functools.partial(feed_body, math.gcd(here, 256), paired),
        out_shape=(
            jax.ShapeDtypeStruct((here, cols), BF16),
            jax.ShapeDtypeStruct((here, cols), F32),
        ),
        in_specs=[smem] + [vmem] * (len(mixed) + 6),
        out_specs=(vmem, vmem),
        name="feed",
    )(meta, *mixed, own_x, out_weight, gains, shifts, ffn_in, ffn_out)


def swap(array, axis):
    return lax.ppermute(array, axis, [(0, 1), (1, 0)])


def on_device(
    node_state,
    norm_gains,
    norm_shifts,
    query_weight,
    key_weight,
    value_weight,
    out_weight,
    ffn_in,
    ffn_out,
    live_counts,
    send_rows,
    tile_keys,
    tile_bits,
):
    n_chan = lax.axis_size("chan")
    n_sub = lax.axis_size("sub")
    n_space = lax.axis_size("space")
    paired = n_chan == 2 and n_sub == 2
    chan_at = lax.axis_index("chan")
    sub_at = lax.axis_index("sub")
    node_count, local_cols = node_state.shape
    here = node_count // n_sub
    meta = jnp.stack([chan_at, sub_at]).astype(jnp.int32)

    up = [(i, i + 1) for i in range(n_space - 1)]
    down = [(i + 1, i) for i in range(n_space - 1)]
    if paired:
        across = swap(node_state, "chan")
    upward, downward = pick_rows(send_rows[0], node_state)
    lower = lax.ppermute(upward, "space", up)
    upper = lax.ppermute(downward, "space", down)
    halo = jnp.concatenate([lower, upper], axis=0)
    if paired:
        halo_across = swap(halo, "chan")
        mains = [node_state, swap(node_state, "sub"), across, swap(across, "sub")]
        halos = [halo, swap(halo, "sub"), halo_across, swap(halo_across, "sub")]
    else:
        mains = [lax.all_gather(node_state, ("chan", "sub"), axis=1, tiled=True)]
        halos = [lax.all_gather(halo, ("chan", "sub"), axis=1, tiled=True)]
    queries, keys, values_t, own_x = project(
        meta, mains, halos, norm_gains, norm_shifts, query_weight, key_weight, value_weight.T, here
    )
    attended = attend(meta, live_counts, tile_keys, queries, tile_bits, keys, values_t)
    if paired:
        mixed = [attended, swap(attended, "chan")]
    else:
        mixed = [lax.all_gather(attended, "chan", axis=1, tiled=True)]
    send, keep = feed(meta, mixed, own_x, out_weight, norm_gains, norm_shifts, ffn_in, ffn_out)
    if paired:
        total = keep + swap(send, "chan").astype(F32)
    else:
        width = keep.shape[1] // n_chan
        kept = lax.dynamic_slice_in_dim(keep, chan_at * width, width, 1)
        total = kept + lax.psum_scatter(send, "chan", scatter_dimension=1, tiled=True).astype(F32)
    position = sub_at * here + jnp.arange(here, dtype=jnp.int32)
    result = jnp.where((position < live_counts[0])[:, None], total, 0.0).astype(BF16)
    if paired:
        first = sub_at == 0
        mine = jnp.where(first, result[:, :local_cols], result[:, local_cols:])
        theirs = swap(jnp.where(first, result[:, local_cols:], result[:, :local_cols]), "sub")
        return jnp.concatenate(
            [jnp.where(first, mine, theirs), jnp.where(first, theirs, mine)], axis=0
        )
    return lax.all_to_all(result, "sub", split_axis=1, concat_axis=0, tiled=True)


def solution(mesh):
    in_specs = (
        P(("ens", "space"), ("chan", "sub")),
        P(),
        P(),
        P(None, "chan"),
        P(None, "chan"),
        P(None, "chan"),
        P(),
        P("chan", None),
        P("chan", None),
        P("space"),
        P("space", None, None),
        P("space", None),
        P("space", None, None, None),
    )
    out_specs = P(("ens", "space"), ("chan", "sub"))
    return jax.shard_map(
        on_device, mesh=mesh, in_specs=in_specs, out_specs=out_specs, check_vma=False
    )
```

```python
import functools
import math

import jax
import jax.numpy as jnp
from jax import lax
from jax.experimental import pallas as pl
from jax.experimental.pallas import tpu as pltpu
from jax.sharding import PartitionSpec as P


HD = 64


NORM_EPS = 1e-05
F32 = jnp.float32
BF16 = jnp.bfloat16
NT = (((1,), (1,)), ((), ()))
NN = (((1,), (0,)), ((), ()))


def dot(a, b, dims=NN):
    return lax.dot_general(a, b, dims, preferred_element_type=F32)


def normalize_rows(source, gain_row, shift_row):
    row_mean = jnp.mean(source, axis=-1, keepdims=True)
    spread = jnp.mean(source * source, axis=-1, keepdims=True) - row_mean * row_mean
    return (source - row_mean) * lax.rsqrt(spread + NORM_EPS) * gain_row + shift_row


def pick_body(list_ref, x_ref, up_ref, down_ref):
    rows = x_ref.shape[0]
    width = list_ref.shape[-1]
    source = x_ref[...]
    node = lax.broadcasted_iota(jnp.int32, (rows, width), 0)
    for at, out in ((1, up_ref), (0, down_ref)):
        hot = (node == list_ref[at : at + 1, :]).astype(F32).astype(BF16)
        out[...] = lax.dot_general(
            hot, source, (((0,), (0,)), ((), ())), preferred_element_type=F32
        ).astype(BF16)


def pick_rows(send_list, source):
    shape = jax.ShapeDtypeStruct((send_list.shape[1], source.shape[1]), source.dtype)
    return pl.pallas_call(pick_body, out_shape=(shape, shape), name="pick_rows")(send_list, source)


def vmem_limit(*shapes):
    total = 8 * 2**20
    for shape in shapes:
        rows, lanes = math.prod(shape.shape[:-1]), -(-shape.shape[-1] // 128) * 128
        total += -(-rows // 16) * 16 * lanes * jnp.dtype(shape.dtype).itemsize
    return min(total, 60 * 2**20)


def gather_pieces(chan_at, sub_at, pieces, xs_ref):
    cols = pieces[0].shape[1]
    for i, piece in enumerate(pieces):
        if len(pieces) == 1:
            place = slice(None)
        else:
            chan_of = chan_at if i < 2 else 1 - chan_at
            sub_of = sub_at if i % 2 == 0 else 1 - sub_at
            place = pl.ds(pl.multiple_of((chan_of * 2 + sub_of) * cols, cols), cols)
        xs_ref[:, place] = piece[...]


def project_body(chunk, count, chan_ref, sub_ref, *refs):
    pieces = refs[:count]
    gain_ref, shift_ref, wqt_ref, wk_ref, wvt_ref = refs[count : count + 5]
    qt_ref, k_ref, vt_ref, own_ref, xs_ref, ns_ref = refs[count + 5 :]
    sub_at = sub_ref[0]
    gather_pieces(chan_ref[0], sub_at, pieces, xs_ref)
    gain, shift = gain_ref[0:1, :], shift_ref[0:1, :]

    def step(j, carry):
        at = pl.ds(pl.multiple_of(j * chunk, chunk), chunk)
        normed = normalize_rows(xs_ref[at, :].astype(F32), gain, shift).astype(BF16)
        ns_ref[at, :] = normed
        k_ref[at, :] = dot(normed, wk_ref[...]).astype(BF16)
        vt_ref[:, at] = dot(wvt_ref[...], normed, NT).astype(BF16)
        return carry

    lax.fori_loop(0, xs_ref.shape[0] // chunk, step, 0, unroll=True)
    here = own_ref.shape[0]
    own = pl.ds(pl.multiple_of(sub_at * here, here), here)
    own_ref[...] = xs_ref[own, :]
    scale = 1.0 / math.sqrt(HD)
    qt = dot(wqt_ref[...], ns_ref[own, :], NT).astype(BF16)
    qt_ref[...] = (qt.astype(F32) * scale).astype(BF16)


def project(place, mains, gains, shifts, wqt, wk, wvt, here):
    rows = mains[0].shape[0]
    width = gains.shape[1]
    head_cols = wk.shape[1]
    vmem = pl.BlockSpec(memory_space=pltpu.VMEM)
    smem = pl.BlockSpec(memory_space=pltpu.SMEM)
    wide = jax.ShapeDtypeStruct((rows, width), BF16)
    outs = (
        jax.ShapeDtypeStruct((head_cols, here), BF16),
        jax.ShapeDtypeStruct((rows, head_cols), BF16),
        jax.ShapeDtypeStruct((head_cols, rows), BF16),
        jax.ShapeDtypeStruct((here, width), BF16),
    )
    return pl.pallas_call(
        functools.partial(project_body, math.gcd(rows, 256), len(mains)),
        out_shape=outs,
        in_specs=[smem] * 2 + [vmem] * (len(mains) + 5),
        out_specs=(vmem,) * 4,
        scratch_shapes=[pltpu.VMEM((rows, width), BF16)] * 2,
        compiler_params=pltpu.CompilerParams(
            vmem_limit_bytes=vmem_limit(wide, wide, *mains, *outs, wqt, wk, wvt)
        ),
        name="project",
    )(*place, *mains, gains, shifts, wqt, wk, wvt)


def extend_body(count, chan_ref, sub_ref, *refs):
    pieces = refs[:count]
    gain_ref, shift_ref, wk_ref, wvt_ref, k_ref, vt_ref = refs[count : count + 6]
    ke_ref, vte_ref, xs_ref = refs[count + 6 :]
    rows = k_ref.shape[0]
    gather_pieces(chan_ref[0], sub_ref[0], pieces, xs_ref)
    ke_ref[:rows, :] = k_ref[...]
    vte_ref[:, :rows] = vt_ref[...]
    gain, shift = gain_ref[0:1, :], shift_ref[0:1, :]
    normed = normalize_rows(xs_ref[...].astype(F32), gain, shift).astype(BF16)
    ke_ref[rows:, :] = dot(normed, wk_ref[...]).astype(BF16)
    vte_ref[:, rows:] = dot(wvt_ref[...], normed, NT).astype(BF16)


def extend(place, halos, gains, shifts, wk, wvt, keys, values_t):
    rows, head_cols = keys.shape
    extra = halos[0].shape[0]
    vmem = pl.BlockSpec(memory_space=pltpu.VMEM)
    smem = pl.BlockSpec(memory_space=pltpu.SMEM)
    outs = (
        jax.ShapeDtypeStruct((rows + extra, head_cols), BF16),
        jax.ShapeDtypeStruct((head_cols, rows + extra), BF16),
    )
    wide = jax.ShapeDtypeStruct((extra, gains.shape[1]), BF16)
    return pl.pallas_call(
        functools.partial(extend_body, len(halos)),
        out_shape=outs,
        in_specs=[smem] * 2 + [vmem] * (len(halos) + 6),
        out_specs=(vmem, vmem),
        scratch_shapes=[pltpu.VMEM(wide.shape, BF16)],
        compiler_params=pltpu.CompilerParams(
            vmem_limit_bytes=vmem_limit(wide, *halos, *outs, keys, values_t, wk, wvt)
        ),
        name="extend",
    )(*place, *halos, gains, shifts, wk, wvt, keys, values_t)


def attend_body(
    first, per_sub, blocks_own, sub_ref, live_ref, id_ref, qt_ref, bit_ref, k_ref, vt_ref,
    out_ref, s_ref,
):
    slot_count, word_count, tile = bit_ref.shape[1:]
    head_cols = qt_ref.shape[0]
    heads = head_cols // HD
    block = sub_ref[0] * per_sub + first + pl.program_id(0)
    live = live_ref[0]
    qt = qt_ref[...]
    row = lax.broadcasted_iota(jnp.int32, (head_cols, tile), 0)
    spread = jnp.concatenate(
        [jnp.where(row // HD == h, qt, jnp.zeros_like(qt)) for h in range(heads)], axis=1
    )
    key_at = lax.broadcasted_iota(jnp.int32, (tile, tile), 0)
    query_at = lax.broadcasted_iota(jnp.int32, (tile, tile), 1)
    per_word = tile // word_count
    bit_at = lax.broadcasted_iota(jnp.int32, (per_word, tile), 0)
    per_dot = math.gcd(slot_count, 2)
    peaks = [None] * heads
    starts = [pl.multiple_of(id_ref[block, t] * tile, tile) for t in range(slot_count)]
    for base in range(0, slot_count, per_dot):
        block_keys = [k_ref[pl.ds(starts[base + i], tile), :] for i in range(per_dot)]
        scores = dot(jnp.concatenate(block_keys, axis=0), spread)
        for i in range(per_dot):
            t = base + i
            key_id = id_ref[block, t]
            limit = jnp.where(key_id >= blocks_own, tile, live - key_id * tile)
            usable = key_at < limit
            if t == 0:
                usable = usable | (key_at == query_at)
            words = jnp.concatenate(
                [
                    jnp.right_shift(
                        jnp.broadcast_to(bit_ref[0, t, w : w + 1, :], (per_word, tile)), bit_at
                    )
                    & 1
                    for w in range(word_count)
                ],
                axis=0,
            )
            allowed = (words == 1) & usable
            for h in range(heads):
                cols = slice(h * tile, (h + 1) * tile)
                part = jnp.where(allowed, scores[i * tile : (i + 1) * tile, cols], -jnp.inf)
                s_ref[t * tile : (t + 1) * tile, cols] = part
                top = jnp.max(part.reshape(tile // 8, 8, tile), axis=0)
                peaks[h] = top if peaks[h] is None else jnp.maximum(peaks[h], top)
    peak = jnp.max(jnp.concatenate(peaks, axis=1), axis=0, keepdims=True)
    group = math.gcd(heads, 2)
    mixed = [None] * (heads // group)
    total = None
    for t in range(0, slot_count, per_dot):
        weights = jnp.exp(s_ref[t * tile : (t + per_dot) * tile, :] - peak)
        part = jnp.sum(weights.reshape(per_dot * tile // 8, 8, heads * tile), axis=0)
        total = part if total is None else total + part
        weights = weights.astype(BF16)
        for g in range(heads // group):
            values = jnp.concatenate(
                [
                    vt_ref[g * group * HD : (g + 1) * group * HD, pl.ds(starts[t + i], tile)]
                    for i in range(per_dot)
                ],
                axis=1,
            )
            add = dot(values, weights[:, g * group * tile : (g + 1) * group * tile])
            mixed[g] = add if mixed[g] is None else mixed[g] + add
    total = jnp.sum(total, axis=0, keepdims=True)
    pieces = []
    for h in range(heads):
        g, i = divmod(h, group)
        own = mixed[g][i * HD : (i + 1) * HD, i * tile : (i + 1) * tile]
        pieces.append(own / total[:, h * tile : (h + 1) * tile])
    out_ref[...] = jnp.concatenate(pieces, axis=0).T.astype(BF16)


def attend(sub_id, live_counts, tile_keys, queries_t, tile_bits, keys, values_t, first, count):
    blocks_own, slot_count, word_count, tile = tile_bits.shape
    head_cols, here = queries_t.shape
    total = keys.shape[0]
    per_sub = here // tile
    heads = head_cols // HD
    scratch = jax.ShapeDtypeStruct((slot_count * tile, heads * tile), F32)
    return pl.pallas_call(
        functools.partial(attend_body, first, per_sub, blocks_own),
        out_shape=jax.ShapeDtypeStruct((count * tile, head_cols), BF16),
        grid_spec=pltpu.PrefetchScalarGridSpec(
            num_scalar_prefetch=3,
            grid=(count,),
            in_specs=[
                pl.BlockSpec((head_cols, tile), lambda i, m, n, k: (0, first + i)),
                pl.BlockSpec(
                    (1, slot_count, word_count, tile),
                    lambda i, m, n, k: (m[0] * per_sub + first + i, 0, 0, 0),
                ),
                pl.BlockSpec((total, head_cols), lambda i, m, n, k: (0, 0)),
                pl.BlockSpec((head_cols, total), lambda i, m, n, k: (0, 0)),
            ],
            out_specs=pl.BlockSpec((tile, head_cols), lambda i, m, n, k: (i, 0)),
            scratch_shapes=[pltpu.VMEM(scratch.shape, F32)],
        ),
        compiler_params=pltpu.CompilerParams(
            vmem_limit_bytes=vmem_limit(scratch, scratch, keys, keys, values_t, values_t)
        ),
        name="attend",
    )(sub_id, live_counts, tile_keys, queries_t, tile_bits, keys, values_t)


def feed_body(first_row, chunk, paired, chan_ref, *refs):
    count = 2 if paired else 1
    mixed = refs[:count]
    x_ref, wo_ref, gain_ref, shift_ref, in_ref, out_w_ref, send_ref, keep_ref = refs[count:]
    chan_at = chan_ref[0]
    width = x_ref.shape[1]
    here = mixed[0].shape[0]
    gain, shift = gain_ref[1:2, :], shift_ref[1:2, :]

    def step(j, carry):
        at = pl.ds(pl.multiple_of(j * chunk, chunk), chunk)
        after = x_ref[pl.ds(pl.multiple_of(first_row + j * chunk, chunk), chunk), :].astype(F32)
        for i in range(count):
            cols = mixed[i].shape[1]
            if paired:
                chan_of = chan_at if i == 0 else 1 - chan_at
                weight = wo_ref[pl.ds(pl.multiple_of(chan_of * cols, cols), cols), :]
            else:
                weight = wo_ref[...]
            after = after + dot(mixed[i][at, :], weight)
        normed = normalize_rows(after, gain, shift).astype(BF16)
        hidden = jax.nn.gelu(dot(normed, in_ref[...], NT)).astype(BF16)
        update = dot(hidden, out_w_ref[...])
        if paired:
            half = width // 2
            first = chan_at == 0
            send_ref[at, :] = jnp.where(first, update[:, half:], update[:, :half]).astype(BF16)
            both = after + update
            keep_ref[at, :] = jnp.where(first, both[:, :half], both[:, half:])
        else:
            send_ref[at, :] = update.astype(BF16)
            keep_ref[at, :] = after
        return carry

    lax.fori_loop(0, here // chunk, step, 0)


def feed(chan_id, mixed, own_x, out_weight, gains, shifts, ffn_in, ffn_out, first_row):
    paired = len(mixed) == 2
    here, width = mixed[0].shape[0], own_x.shape[1]
    cols = width // 2 if paired else width
    vmem = pl.BlockSpec(memory_space=pltpu.VMEM)
    smem = pl.BlockSpec(memory_space=pltpu.SMEM)
    outs = (jax.ShapeDtypeStruct((here, cols), BF16), jax.ShapeDtypeStruct((here, cols), F32))
    return pl.pallas_call(
        functools.partial(feed_body, first_row, math.gcd(here, 256), paired),
        out_shape=outs,
        in_specs=[smem] + [vmem] * (len(mixed) + 6),
        out_specs=(vmem, vmem),
        compiler_params=pltpu.CompilerParams(
            vmem_limit_bytes=vmem_limit(*mixed, *outs, own_x, out_weight, ffn_in, ffn_out)
        ),
        name="feed",
    )(chan_id, *mixed, own_x, out_weight, gains, shifts, ffn_in, ffn_out)


def swap(array, axis):
    return lax.ppermute(array, axis, [(0, 1), (1, 0)])


def on_device(
    node_state,
    norm_gains,
    norm_shifts,
    query_weight,
    key_weight,
    value_weight,
    out_weight,
    ffn_in,
    ffn_out,
    live_counts,
    send_rows,
    tile_keys,
    tile_bits,
):
    n_chan = lax.axis_size("chan")
    n_sub = lax.axis_size("sub")
    n_space = lax.axis_size("space")
    paired = n_chan == 2 and n_sub == 2
    chan_at = lax.axis_index("chan")
    sub_at = lax.axis_index("sub")
    node_count, local_cols = node_state.shape
    tile = tile_bits.shape[-1]
    here = node_count // n_sub
    place = (chan_at.astype(jnp.int32).reshape(1), sub_at.astype(jnp.int32).reshape(1))
    up = [(i, i + 1) for i in range(n_space - 1)]
    down = [(i + 1, i) for i in range(n_space - 1)]

    if paired:
        across = swap(node_state, "chan")
        mains = [node_state, swap(node_state, "sub"), across, swap(across, "sub")]
    else:
        mains = [lax.all_gather(node_state, ("chan", "sub"), axis=1, tiled=True)]
    upward, downward = pick_rows(send_rows[0], node_state)
    lower = lax.ppermute(upward, "space", up)
    upper = lax.ppermute(downward, "space", down)
    halo = jnp.concatenate([lower, upper], axis=0)
    if paired:
        halo_across = swap(halo, "chan")
        halos = [halo, swap(halo, "sub"), halo_across, swap(halo_across, "sub")]
    else:
        halos = [lax.all_gather(halo, ("chan", "sub"), axis=1, tiled=True)]
    values_w = value_weight.T
    queries_t, keys, values_t, own_x = project(
        place, mains, norm_gains, norm_shifts, query_weight.T, key_weight, values_w, here
    )
    keys, values_t = extend(
        place, halos, norm_gains, norm_shifts, key_weight, values_w, keys, values_t
    )
    blocks_here = here // tile
    parts = math.gcd(blocks_here, 2)
    count = blocks_here // parts
    attended = []
    for i in range(parts):
        attended.append(
            attend(
                place[1], live_counts, tile_keys, queries_t, tile_bits, keys, values_t,
                i * count, count,
            )
        )
    finals = []
    for i in range(parts):
        if paired:
            mixed = [attended[i], swap(attended[i], "chan")]
        else:
            mixed = [lax.all_gather(attended[i], "chan", axis=1, tiled=True)]
        first_row = i * count * tile
        send, keep = feed(
            place[0], mixed, own_x, out_weight, norm_gains, norm_shifts, ffn_in, ffn_out,
            first_row,
        )
        if paired:
            total = keep + swap(send, "chan").astype(F32)
        else:
            width = keep.shape[1] // n_chan
            kept = lax.dynamic_slice_in_dim(keep, chan_at * width, width, 1)
            added = lax.psum_scatter(send, "chan", scatter_dimension=1, tiled=True)
            total = kept + added.astype(F32)
        position = sub_at * here + first_row + jnp.arange(total.shape[0], dtype=jnp.int32)
        finals.append(jnp.where((position < live_counts[0])[:, None], total, 0.0).astype(BF16))
    if paired:
        first = sub_at == 0
        mine, theirs = [], []
        for result in finals:
            left, right = result[:, :local_cols], result[:, local_cols:]
            mine.append(jnp.where(first, left, right))
            theirs.append(swap(jnp.where(first, right, left), "sub"))
        low = [jnp.where(first, a, b) for a, b in zip(mine, theirs)]
        high = [jnp.where(first, b, a) for a, b in zip(mine, theirs)]
        return jnp.concatenate(low + high, axis=0)
    result = jnp.concatenate(finals, axis=0)
    return lax.all_to_all(result, "sub", split_axis=1, concat_axis=0, tiled=True)


def solution(mesh):
    in_specs = (
        P(("ens", "space"), ("chan", "sub")),
        P(),
        P(),
        P(None, "chan"),
        P(None, "chan"),
        P(None, "chan"),
        P(),
        P("chan", None),
        P("chan", None),
        P("space"),
        P("space", None, None),
        P("space", None),
        P("space", None, None, None),
    )
    out_specs = P(("ens", "space"), ("chan", "sub"))

    return jax.shard_map(
        on_device, mesh=mesh, in_specs=in_specs, out_specs=out_specs, check_vma=False
    )
```

```python
import functools
import math

import jax
import jax.numpy as jnp
from jax import lax
from jax.experimental import pallas as pl
from jax.experimental.pallas import tpu as pltpu
from jax.sharding import PartitionSpec as P


HD = 64


NORM_EPS = 1e-05
F32 = jnp.float32
BF16 = jnp.bfloat16
NT = (((1,), (1,)), ((), ()))
NN = (((1,), (0,)), ((), ()))


def dot(a, b, dims=NN):
    return lax.dot_general(a, b, dims, preferred_element_type=F32)


def normalize_rows(source, gain_row, shift_row):
    row_mean = jnp.mean(source, axis=-1, keepdims=True)
    spread = jnp.mean(source * source, axis=-1, keepdims=True) - row_mean * row_mean
    return (source - row_mean) * lax.rsqrt(spread + NORM_EPS) * gain_row + shift_row


def pick_body(list_ref, x_ref, up_ref, down_ref):
    rows = x_ref.shape[0]
    width = list_ref.shape[-1]
    source = x_ref[...]
    node = lax.broadcasted_iota(jnp.int32, (rows, width), 0)
    for at, out in ((1, up_ref), (0, down_ref)):
        hot = (node == list_ref[at : at + 1, :]).astype(F32).astype(BF16)
        out[...] = lax.dot_general(
            hot, source, (((0,), (0,)), ((), ())), preferred_element_type=F32
        ).astype(BF16)


def pick_rows(send_list, source):
    shape = jax.ShapeDtypeStruct((send_list.shape[1], source.shape[1]), source.dtype)
    wide = jax.ShapeDtypeStruct((source.shape[0], 4 * shape.shape[0]), F32)
    return pl.pallas_call(
        pick_body,
        out_shape=(shape, shape),
        compiler_params=pltpu.CompilerParams(vmem_limit_bytes=vmem_limit(wide, source)),
        name="pick_rows",
    )(send_list, source)


def flip_body(a_ref, b_ref, at_ref, bt_ref):
    at_ref[...] = a_ref[...].T
    bt_ref[...] = b_ref[...].T


def flip(a, b):
    shape = jax.ShapeDtypeStruct(a.shape[::-1], a.dtype)
    return pl.pallas_call(
        flip_body,
        out_shape=(shape, shape),
        compiler_params=pltpu.CompilerParams(vmem_limit_bytes=vmem_limit(a, b, shape, shape)),
        name="flip",
    )(a, b)


def vmem_limit(*shapes):
    total = 8 * 2**20
    for shape in shapes:
        rows, lanes = math.prod(shape.shape[:-1]), -(-shape.shape[-1] // 128) * 128
        total += -(-rows // 16) * 16 * lanes * jnp.dtype(shape.dtype).itemsize
    return min(total, 60 * 2**20)


def gather_pieces(chan_at, sub_at, pieces, xs_ref):
    cols = pieces[0].shape[1]
    for i, piece in enumerate(pieces):
        if len(pieces) == 1:
            place = slice(None)
        else:
            chan_of = chan_at if i < 2 else 1 - chan_at
            sub_of = sub_at if i % 2 == 0 else 1 - sub_at
            place = pl.ds(pl.multiple_of((chan_of * 2 + sub_of) * cols, cols), cols)
        xs_ref[:, place] = piece[...]


def project_body(chunk, count, chan_ref, sub_ref, *refs):
    pieces = refs[:count]
    gain_ref, shift_ref, wqt_ref, wk_ref, wvt_ref = refs[count : count + 5]
    qt_ref, k_ref, vt_ref, own_ref, xs_ref, ns_ref = refs[count + 5 :]
    sub_at = sub_ref[0]
    gather_pieces(chan_ref[0], sub_at, pieces, xs_ref)
    gain, shift = gain_ref[0:1, :], shift_ref[0:1, :]

    def step(j, carry):
        at = pl.ds(pl.multiple_of(j * chunk, chunk), chunk)
        normed = normalize_rows(xs_ref[at, :].astype(F32), gain, shift).astype(BF16)
        ns_ref[at, :] = normed
        k_ref[at, :] = dot(normed, wk_ref[...]).astype(BF16)
        vt_ref[:, at] = dot(wvt_ref[...], normed, NT).astype(BF16)
        return carry

    lax.fori_loop(0, xs_ref.shape[0] // chunk, step, 0, unroll=True)
    here = own_ref.shape[0]
    own = pl.ds(pl.multiple_of(sub_at * here, here), here)
    own_ref[...] = xs_ref[own, :]
    scale = 1.0 / math.sqrt(HD)
    qt = dot(wqt_ref[...], ns_ref[own, :], NT).astype(BF16)
    qt_ref[...] = (qt.astype(F32) * scale).astype(BF16)


def project(place, mains, gains, shifts, wqt, wk, wvt, here):
    rows = mains[0].shape[0]
    width = gains.shape[1]
    head_cols = wk.shape[1]
    vmem = pl.BlockSpec(memory_space=pltpu.VMEM)
    smem = pl.BlockSpec(memory_space=pltpu.SMEM)
    wide = jax.ShapeDtypeStruct((rows, width), BF16)
    outs = (
        jax.ShapeDtypeStruct((head_cols, here), BF16),
        jax.ShapeDtypeStruct((rows, head_cols), BF16),
        jax.ShapeDtypeStruct((head_cols, rows), BF16),
        jax.ShapeDtypeStruct((here, width), BF16),
    )
    return pl.pallas_call(
        functools.partial(project_body, math.gcd(rows, 256), len(mains)),
        out_shape=outs,
        in_specs=[smem] * 2 + [vmem] * (len(mains) + 5),
        out_specs=(vmem,) * 4,
        scratch_shapes=[pltpu.VMEM((rows, width), BF16)] * 2,
        compiler_params=pltpu.CompilerParams(
            vmem_limit_bytes=vmem_limit(wide, wide, *mains, *outs, wqt, wk, wvt)
        ),
        name="project",
    )(*place, *mains, gains, shifts, wqt, wk, wvt)


def extend_body(count, chan_ref, sub_ref, *refs):
    pieces = refs[:count]
    gain_ref, shift_ref, wk_ref, wvt_ref, k_ref, vt_ref = refs[count : count + 6]
    ke_ref, vte_ref, xs_ref = refs[count + 6 :]
    rows = k_ref.shape[0]
    gather_pieces(chan_ref[0], sub_ref[0], pieces, xs_ref)
    ke_ref[:rows, :] = k_ref[...]
    vte_ref[:, :rows] = vt_ref[...]
    gain, shift = gain_ref[0:1, :], shift_ref[0:1, :]
    normed = normalize_rows(xs_ref[...].astype(F32), gain, shift).astype(BF16)
    ke_ref[rows:, :] = dot(normed, wk_ref[...]).astype(BF16)
    vte_ref[:, rows:] = dot(wvt_ref[...], normed, NT).astype(BF16)


def extend(place, halos, gains, shifts, wk, wvt, keys, values_t):
    rows, head_cols = keys.shape
    extra = halos[0].shape[0]
    vmem = pl.BlockSpec(memory_space=pltpu.VMEM)
    smem = pl.BlockSpec(memory_space=pltpu.SMEM)
    outs = (
        jax.ShapeDtypeStruct((rows + extra, head_cols), BF16),
        jax.ShapeDtypeStruct((head_cols, rows + extra), BF16),
    )
    wide = jax.ShapeDtypeStruct((extra, gains.shape[1]), BF16)
    return pl.pallas_call(
        functools.partial(extend_body, len(halos)),
        out_shape=outs,
        in_specs=[smem] * 2 + [vmem] * (len(halos) + 6),
        out_specs=(vmem, vmem),
        scratch_shapes=[pltpu.VMEM(wide.shape, BF16)],
        compiler_params=pltpu.CompilerParams(
            vmem_limit_bytes=vmem_limit(wide, *halos, *outs, keys, values_t, wk, wvt)
        ),
        name="extend",
    )(*place, *halos, gains, shifts, wk, wvt, keys, values_t)


def attend_body(
    first, per_sub, blocks_own, sub_ref, live_ref, id_ref, qt_ref, bit_ref, k_ref, vt_ref,
    out_ref, s_ref,
):
    tile = bit_ref.shape[-1]
    count = out_ref.shape[0] // tile
    slots = s_ref.shape[0]

    def step(j, carry):
        for i in range(slots):
            attend_block(
                first, per_sub, blocks_own, j * slots + i, sub_ref, live_ref, id_ref, qt_ref,
                bit_ref, k_ref, vt_ref, out_ref, s_ref.at[i],
            )
        return carry

    if count == slots:
        step(0, 0)
    else:
        lax.fori_loop(0, count // slots, step, 0)


def attend_block(
    first, per_sub, blocks_own, at, sub_ref, live_ref, id_ref, qt_ref, bit_ref, k_ref, vt_ref,
    out_ref, s_ref,
):
    slot_count, word_count, tile = bit_ref.shape[1:]
    head_cols = qt_ref.shape[0]
    heads = head_cols // HD
    block = sub_ref[0] * per_sub + first + at
    live = live_ref[0]
    q_at = (first + at) * tile
    out_at = at * tile
    if not isinstance(at, int):
        q_at, out_at = pl.multiple_of(q_at, tile), pl.multiple_of(out_at, tile)
    qt = qt_ref[:, pl.ds(q_at, tile)]
    row = lax.broadcasted_iota(jnp.int32, (head_cols, tile), 0)
    spread = jnp.concatenate(
        [jnp.where(row // HD == h, qt, jnp.zeros_like(qt)) for h in range(heads)], axis=1
    )
    key_at = lax.broadcasted_iota(jnp.int32, (tile, tile), 0)
    query_at = lax.broadcasted_iota(jnp.int32, (tile, tile), 1)
    per_word = tile // word_count
    bit_at = lax.broadcasted_iota(jnp.int32, (per_word, tile), 0)
    per_dot = math.gcd(slot_count, 2)
    peaks = [None] * heads
    starts = [pl.multiple_of(id_ref[block, t] * tile, tile) for t in range(slot_count)]
    for base in range(0, slot_count, per_dot):
        block_keys = [k_ref[pl.ds(starts[base + i], tile), :] for i in range(per_dot)]
        scores = dot(jnp.concatenate(block_keys, axis=0), spread)
        for i in range(per_dot):
            t = base + i
            key_id = id_ref[block, t]
            limit = jnp.where(key_id >= blocks_own, tile, live - key_id * tile)
            usable = key_at < limit
            if t == 0:
                usable = usable | (key_at == query_at)
            words = jnp.concatenate(
                [
                    jnp.right_shift(
                        jnp.broadcast_to(bit_ref[block, t, w : w + 1, :], (per_word, tile)), bit_at
                    )
                    & 1
                    for w in range(word_count)
                ],
                axis=0,
            )
            allowed = (words == 1) & usable
            for h in range(heads):
                cols = slice(h * tile, (h + 1) * tile)
                part = jnp.where(allowed, scores[i * tile : (i + 1) * tile, cols], -jnp.inf)
                s_ref[t * tile : (t + 1) * tile, cols] = part
                top = jnp.max(part.reshape(tile // 8, 8, tile), axis=0)
                peaks[h] = top if peaks[h] is None else jnp.maximum(peaks[h], top)
    peak = jnp.max(jnp.concatenate(peaks, axis=1), axis=0, keepdims=True)
    group = math.gcd(heads, 2)
    mixed = [None] * (heads // group)
    total = None
    for t in range(0, slot_count, per_dot):
        weights = jnp.exp(s_ref[t * tile : (t + per_dot) * tile, :] - peak)
        part = jnp.sum(weights.reshape(per_dot * tile // 8, 8, heads * tile), axis=0)
        total = part if total is None else total + part
        weights = weights.astype(BF16)
        for g in range(heads // group):
            values = jnp.concatenate(
                [
                    vt_ref[g * group * HD : (g + 1) * group * HD, pl.ds(starts[t + i], tile)]
                    for i in range(per_dot)
                ],
                axis=1,
            )
            add = dot(values, weights[:, g * group * tile : (g + 1) * group * tile])
            mixed[g] = add if mixed[g] is None else mixed[g] + add
    total = jnp.sum(total, axis=0, keepdims=True)
    pieces = []
    for h in range(heads):
        g, i = divmod(h, group)
        own = mixed[g][i * HD : (i + 1) * HD, i * tile : (i + 1) * tile]
        pieces.append(own / total[:, h * tile : (h + 1) * tile])
    out_ref[pl.ds(out_at, tile), :] = jnp.concatenate(pieces, axis=0).T.astype(BF16)


def attend(sub_id, live_counts, tile_keys, queries_t, tile_bits, keys, values_t, first, count):
    blocks_own, slot_count, _, tile = tile_bits.shape
    head_cols, here = queries_t.shape
    per_sub = here // tile
    heads = head_cols // HD
    scratch = jax.ShapeDtypeStruct((math.gcd(count, 2), slot_count * tile, heads * tile), F32)
    vmem = pl.BlockSpec(memory_space=pltpu.VMEM)
    smem = pl.BlockSpec(memory_space=pltpu.SMEM)
    out = jax.ShapeDtypeStruct((count * tile, head_cols), BF16)
    bits = jax.ShapeDtypeStruct((blocks_own, slot_count, 8, tile), jnp.int32)
    return pl.pallas_call(
        functools.partial(attend_body, first, per_sub, blocks_own),
        out_shape=out,
        in_specs=[smem] * 3 + [vmem] * 4,
        out_specs=vmem,
        scratch_shapes=[pltpu.VMEM(scratch.shape, F32)],
        compiler_params=pltpu.CompilerParams(
            vmem_limit_bytes=vmem_limit(scratch, keys, values_t, queries_t, bits, out)
        ),
        name="attend",
    )(sub_id, live_counts, tile_keys, queries_t, tile_bits, keys, values_t)


def feed_body(first_row, chunk, paired, chan_ref, *refs):
    count = 2 if paired else 1
    mixed = refs[:count]
    x_ref, wo_ref, gain_ref, shift_ref, in_ref, out_w_ref, send_ref, keep_ref = refs[count:]
    chan_at = chan_ref[0]
    width = x_ref.shape[1]
    here = mixed[0].shape[0]
    gain, shift = gain_ref[1:2, :], shift_ref[1:2, :]

    def step(j, carry):
        at = pl.ds(pl.multiple_of(j * chunk, chunk), chunk)
        after = x_ref[pl.ds(pl.multiple_of(first_row + j * chunk, chunk), chunk), :].astype(F32)
        for i in range(count):
            cols = mixed[i].shape[1]
            if paired:
                chan_of = chan_at if i == 0 else 1 - chan_at
                weight = wo_ref[pl.ds(pl.multiple_of(chan_of * cols, cols), cols), :]
            else:
                weight = wo_ref[...]
            after = after + dot(mixed[i][at, :], weight)
        normed = normalize_rows(after, gain, shift).astype(BF16)
        hidden = jax.nn.gelu(dot(normed, in_ref[...], NT)).astype(BF16)
        update = dot(hidden, out_w_ref[...])
        if paired:
            half = width // 2
            first = chan_at == 0
            send_ref[at, :] = jnp.where(first, update[:, half:], update[:, :half]).astype(BF16)
            both = after + update
            keep_ref[at, :] = jnp.where(first, both[:, :half], both[:, half:])
        else:
            send_ref[at, :] = update.astype(BF16)
            keep_ref[at, :] = after
        return carry

    lax.fori_loop(0, here // chunk, step, 0)


def feed(chan_id, mixed, own_x, out_weight, gains, shifts, ffn_in, ffn_out, first_row):
    paired = len(mixed) == 2
    here, width = mixed[0].shape[0], own_x.shape[1]
    cols = width // 2 if paired else width
    vmem = pl.BlockSpec(memory_space=pltpu.VMEM)
    smem = pl.BlockSpec(memory_space=pltpu.SMEM)
    outs = (jax.ShapeDtypeStruct((here, cols), BF16), jax.ShapeDtypeStruct((here, cols), F32))
    return pl.pallas_call(
        functools.partial(feed_body, first_row, math.gcd(here, 256), paired),
        out_shape=outs,
        in_specs=[smem] + [vmem] * (len(mixed) + 6),
        out_specs=(vmem, vmem),
        compiler_params=pltpu.CompilerParams(
            vmem_limit_bytes=vmem_limit(*mixed, *outs, own_x, out_weight, ffn_in, ffn_out)
        ),
        name="feed",
    )(chan_id, *mixed, own_x, out_weight, gains, shifts, ffn_in, ffn_out)


def swap(array, axis):
    return lax.ppermute(array, axis, [(0, 1), (1, 0)])


def on_device(
    node_state,
    norm_gains,
    norm_shifts,
    query_weight,
    key_weight,
    value_weight,
    out_weight,
    ffn_in,
    ffn_out,
    live_counts,
    send_rows,
    tile_keys,
    tile_bits,
):
    n_chan = lax.axis_size("chan")
    n_sub = lax.axis_size("sub")
    n_space = lax.axis_size("space")
    paired = n_chan == 2 and n_sub == 2
    chan_at = lax.axis_index("chan")
    sub_at = lax.axis_index("sub")
    node_count, local_cols = node_state.shape
    tile = tile_bits.shape[-1]
    here = node_count // n_sub
    place = (chan_at.astype(jnp.int32).reshape(1), sub_at.astype(jnp.int32).reshape(1))
    up = [(i, i + 1) for i in range(n_space - 1)]
    down = [(i + 1, i) for i in range(n_space - 1)]

    if paired:
        across = swap(node_state, "chan")
        mains = [node_state, swap(node_state, "sub"), across, swap(across, "sub")]
    else:
        mains = [lax.all_gather(node_state, ("chan", "sub"), axis=1, tiled=True)]
    upward, downward = pick_rows(send_rows[0], node_state)
    lower = lax.ppermute(upward, "space", up)
    upper = lax.ppermute(downward, "space", down)
    halo = jnp.concatenate([lower, upper], axis=0)
    if paired:
        cross_up = [(2 * i + c, 2 * j + 1 - c) for i, j in up for c in range(2)]
        cross_down = [(2 * i + c, 2 * j + 1 - c) for i, j in down for c in range(2)]
        lower = lax.ppermute(upward, ("space", "chan"), cross_up)
        upper = lax.ppermute(downward, ("space", "chan"), cross_down)
        halo_across = jnp.concatenate([lower, upper], axis=0)
        halo_beside = swap(halo, "sub")
        halo_diagonal = swap(halo_across, "sub")
        halos = [halo, halo_beside, halo_across, halo_diagonal]
    else:
        halos = [lax.all_gather(halo, ("chan", "sub"), axis=1, tiled=True)]
    queries_w, values_w = flip(query_weight, value_weight)
    queries_t, keys, values_t, own_x = project(
        place, mains, norm_gains, norm_shifts, queries_w, key_weight, values_w, here
    )
    keys, values_t = extend(
        place, halos, norm_gains, norm_shifts, key_weight, values_w, keys, values_t
    )
    blocks_here = here // tile
    parts = math.gcd(blocks_here, 2)
    count = blocks_here // parts
    attended = []
    for i in range(parts):
        attended.append(
            attend(
                place[1], live_counts, tile_keys, queries_t, tile_bits, keys, values_t,
                i * count, count,
            )
        )
    finals = []
    for i in range(parts):
        if paired:
            mixed = [attended[i], swap(attended[i], "chan")]
        else:
            mixed = [lax.all_gather(attended[i], "chan", axis=1, tiled=True)]
        first_row = i * count * tile
        send, keep = feed(
            place[0], mixed, own_x, out_weight, norm_gains, norm_shifts, ffn_in, ffn_out,
            first_row,
        )
        if paired:
            total = keep + swap(send, "chan").astype(F32)
        else:
            width = keep.shape[1] // n_chan
            kept = lax.dynamic_slice_in_dim(keep, chan_at * width, width, 1)
            added = lax.psum_scatter(send, "chan", scatter_dimension=1, tiled=True)
            total = kept + added.astype(F32)
        position = sub_at * here + first_row + jnp.arange(total.shape[0], dtype=jnp.int32)
        finals.append(jnp.where((position < live_counts[0])[:, None], total, 0.0).astype(BF16))
    if paired:
        first = sub_at == 0
        mine, theirs = [], []
        for result in finals:
            left, right = result[:, :local_cols], result[:, local_cols:]
            mine.append(jnp.where(first, left, right))
            theirs.append(swap(jnp.where(first, right, left), "sub"))
        low = [jnp.where(first, a, b) for a, b in zip(mine, theirs)]
        high = [jnp.where(first, b, a) for a, b in zip(mine, theirs)]
        return jnp.concatenate(low + high, axis=0)
    result = jnp.concatenate(finals, axis=0)
    return lax.all_to_all(result, "sub", split_axis=1, concat_axis=0, tiled=True)


def solution(mesh):
    in_specs = (
        P(("ens", "space"), ("chan", "sub")),
        P(),
        P(),
        P(None, "chan"),
        P(None, "chan"),
        P(None, "chan"),
        P(),
        P("chan", None),
        P("chan", None),
        P("space"),
        P("space", None, None),
        P("space", None),
        P("space", None, None, None),
    )
    out_specs = P(("ens", "space"), ("chan", "sub"))

    return jax.shard_map(
        on_device, mesh=mesh, in_specs=in_specs, out_specs=out_specs, check_vma=False
    )
```

```python
import functools
import math

import jax
import jax.numpy as jnp
from jax import lax
from jax.experimental import pallas as pl
from jax.experimental.pallas import tpu as pltpu
from jax.sharding import PartitionSpec as P


HD = 64


NORM_EPS = 1e-05
F32 = jnp.float32
BF16 = jnp.bfloat16
NT = (((1,), (1,)), ((), ()))
NN = (((1,), (0,)), ((), ()))


def dot(a, b, dims=NN):
    return lax.dot_general(a, b, dims, preferred_element_type=F32)


def normalize_rows(source, gain_row, shift_row):
    row_mean = jnp.mean(source, axis=-1, keepdims=True)
    spread = jnp.mean(source * source, axis=-1, keepdims=True) - row_mean * row_mean
    return (source - row_mean) * lax.rsqrt(spread + NORM_EPS) * gain_row + shift_row


def pick_body(list_ref, x_ref, up_ref, down_ref):
    rows = x_ref.shape[0]
    width = list_ref.shape[-1]
    source = x_ref[...]
    node = lax.broadcasted_iota(jnp.int32, (rows, width), 0)
    for at, out in ((1, up_ref), (0, down_ref)):
        hot = (node == list_ref[at : at + 1, :]).astype(F32).astype(BF16)
        out[...] = lax.dot_general(
            hot, source, (((0,), (0,)), ((), ())), preferred_element_type=F32
        ).astype(BF16)


def pick_rows(send_list, source):
    shape = jax.ShapeDtypeStruct((send_list.shape[1], source.shape[1]), source.dtype)
    wide = jax.ShapeDtypeStruct((source.shape[0], 4 * shape.shape[0]), F32)
    return pl.pallas_call(
        pick_body,
        out_shape=(shape, shape),
        compiler_params=pltpu.CompilerParams(vmem_limit_bytes=vmem_limit(wide, source)),
        name="pick_rows",
    )(send_list, source)


def flip_body(a_ref, b_ref, at_ref, bt_ref):
    at_ref[...] = a_ref[...].T
    bt_ref[...] = b_ref[...].T


def flip(a, b):
    shape = jax.ShapeDtypeStruct(a.shape[::-1], a.dtype)
    return pl.pallas_call(
        flip_body,
        out_shape=(shape, shape),
        compiler_params=pltpu.CompilerParams(vmem_limit_bytes=vmem_limit(a, b, shape, shape)),
        name="flip",
    )(a, b)


def vmem_limit(*shapes):
    total = 8 * 2**20
    for shape in shapes:
        rows, lanes = math.prod(shape.shape[:-1]), -(-shape.shape[-1] // 128) * 128
        total += -(-rows // 16) * 16 * lanes * jnp.dtype(shape.dtype).itemsize
    return min(total, 60 * 2**20)


def gather_pieces(chan_at, sub_at, pieces, xs_ref):
    cols = pieces[0].shape[1]
    for i, piece in enumerate(pieces):
        if len(pieces) == 1:
            place = slice(None)
        else:
            chan_of = chan_at if i < 2 else 1 - chan_at
            sub_of = sub_at if i % 2 == 0 else 1 - sub_at
            place = pl.ds(pl.multiple_of((chan_of * 2 + sub_of) * cols, cols), cols)
        xs_ref[:, place] = piece[...]


def project_body(chunk, count, chan_ref, sub_ref, *refs):
    pieces = refs[:count]
    gain_ref, shift_ref, wqt_ref, wk_ref, wvt_ref = refs[count : count + 5]
    qt_ref, k_ref, vt_ref, own_ref, xs_ref, ns_ref = refs[count + 5 :]
    sub_at = sub_ref[0]
    gather_pieces(chan_ref[0], sub_at, pieces, xs_ref)
    gain, shift = gain_ref[0:1, :], shift_ref[0:1, :]

    def step(j, carry):
        at = pl.ds(pl.multiple_of(j * chunk, chunk), chunk)
        normed = normalize_rows(xs_ref[at, :].astype(F32), gain, shift).astype(BF16)
        ns_ref[at, :] = normed
        k_ref[at, :] = dot(normed, wk_ref[...]).astype(BF16)
        vt_ref[:, at] = dot(wvt_ref[...], normed, NT).astype(BF16)
        return carry

    lax.fori_loop(0, xs_ref.shape[0] // chunk, step, 0, unroll=True)
    here = own_ref.shape[0]
    own = pl.ds(pl.multiple_of(sub_at * here, here), here)
    own_ref[...] = xs_ref[own, :]
    scale = 1.0 / math.sqrt(HD)
    qt = dot(wqt_ref[...], ns_ref[own, :], NT).astype(BF16)
    qt_ref[...] = (qt.astype(F32) * scale).astype(BF16)


def project(place, mains, gains, shifts, wqt, wk, wvt, here):
    rows = mains[0].shape[0]
    width = gains.shape[1]
    head_cols = wk.shape[1]
    vmem = pl.BlockSpec(memory_space=pltpu.VMEM)
    smem = pl.BlockSpec(memory_space=pltpu.SMEM)
    wide = jax.ShapeDtypeStruct((rows, width), BF16)
    outs = (
        jax.ShapeDtypeStruct((head_cols, here), BF16),
        jax.ShapeDtypeStruct((rows, head_cols), BF16),
        jax.ShapeDtypeStruct((head_cols, rows), BF16),
        jax.ShapeDtypeStruct((here, width), BF16),
    )
    return pl.pallas_call(
        functools.partial(project_body, math.gcd(rows, 256), len(mains)),
        out_shape=outs,
        in_specs=[smem] * 2 + [vmem] * (len(mains) + 5),
        out_specs=(vmem,) * 4,
        scratch_shapes=[pltpu.VMEM((rows, width), BF16)] * 2,
        compiler_params=pltpu.CompilerParams(
            vmem_limit_bytes=vmem_limit(wide, wide, *mains, *outs, wqt, wk, wvt)
        ),
        name="project",
    )(*place, *mains, gains, shifts, wqt, wk, wvt)


def extend_body(count, chan_ref, sub_ref, *refs):
    pieces = refs[:count]
    gain_ref, shift_ref, wk_ref, wvt_ref, k_ref, vt_ref = refs[count : count + 6]
    ke_ref, vte_ref, xs_ref = refs[count + 6 :]
    rows = k_ref.shape[0]
    gather_pieces(chan_ref[0], sub_ref[0], pieces, xs_ref)
    ke_ref[:rows, :] = k_ref[...]
    vte_ref[:, :rows] = vt_ref[...]
    gain, shift = gain_ref[0:1, :], shift_ref[0:1, :]
    normed = normalize_rows(xs_ref[...].astype(F32), gain, shift).astype(BF16)
    ke_ref[rows:, :] = dot(normed, wk_ref[...]).astype(BF16)
    vte_ref[:, rows:] = dot(wvt_ref[...], normed, NT).astype(BF16)


def extend(place, halos, gains, shifts, wk, wvt, keys, values_t):
    rows, head_cols = keys.shape
    extra = halos[0].shape[0]
    vmem = pl.BlockSpec(memory_space=pltpu.VMEM)
    smem = pl.BlockSpec(memory_space=pltpu.SMEM)
    outs = (
        jax.ShapeDtypeStruct((rows + extra, head_cols), BF16),
        jax.ShapeDtypeStruct((head_cols, rows + extra), BF16),
    )
    wide = jax.ShapeDtypeStruct((extra, gains.shape[1]), BF16)
    return pl.pallas_call(
        functools.partial(extend_body, len(halos)),
        out_shape=outs,
        in_specs=[smem] * 2 + [vmem] * (len(halos) + 6),
        out_specs=(vmem, vmem),
        scratch_shapes=[pltpu.VMEM(wide.shape, BF16)],
        compiler_params=pltpu.CompilerParams(
            vmem_limit_bytes=vmem_limit(wide, *halos, *outs, keys, values_t, wk, wvt)
        ),
        name="extend",
    )(*place, *halos, gains, shifts, wk, wvt, keys, values_t)


def attend_body(
    first, per_sub, blocks_own, sub_ref, live_ref, id_ref, qt_ref, bit_ref, k_ref, vt_ref,
    out_ref, s_ref,
):
    tile = bit_ref.shape[-1]
    count = out_ref.shape[0] // tile
    slots = s_ref.shape[0]

    def step(j, carry):
        for i in range(slots):
            attend_block(
                first, per_sub, blocks_own, j * slots + i, sub_ref, live_ref, id_ref, qt_ref,
                bit_ref, k_ref, vt_ref, out_ref, s_ref.at[i],
            )
        return carry

    if count == slots:
        step(0, 0)
    else:
        lax.fori_loop(0, count // slots, step, 0)


def attend_block(
    first, per_sub, blocks_own, at, sub_ref, live_ref, id_ref, qt_ref, bit_ref, k_ref, vt_ref,
    out_ref, s_ref,
):
    slot_count, word_count, tile = bit_ref.shape[1:]
    head_cols = qt_ref.shape[0]
    heads = head_cols // HD
    block = sub_ref[0] * per_sub + first + at
    live = live_ref[0]
    q_at = (first + at) * tile
    out_at = at * tile
    if not isinstance(at, int):
        q_at, out_at = pl.multiple_of(q_at, tile), pl.multiple_of(out_at, tile)
    qt = qt_ref[:, pl.ds(q_at, tile)]
    row = lax.broadcasted_iota(jnp.int32, (head_cols, tile), 0)
    spread = jnp.concatenate(
        [jnp.where(row // HD == h, qt, jnp.zeros_like(qt)) for h in range(heads)], axis=1
    )
    key_at = lax.broadcasted_iota(jnp.int32, (tile, tile), 0)
    query_at = lax.broadcasted_iota(jnp.int32, (tile, tile), 1)
    per_word = tile // word_count
    bit_at = lax.broadcasted_iota(jnp.int32, (per_word, tile), 0)
    per_dot = math.gcd(slot_count, 2)
    peaks = [None] * heads
    starts = [pl.multiple_of(id_ref[block, t] * tile, tile) for t in range(slot_count)]
    for base in range(0, slot_count, per_dot):
        block_keys = [k_ref[pl.ds(starts[base + i], tile), :] for i in range(per_dot)]
        scores = dot(jnp.concatenate(block_keys, axis=0), spread)
        for i in range(per_dot):
            t = base + i
            key_id = id_ref[block, t]
            limit = jnp.where(key_id >= blocks_own, tile, live - key_id * tile)
            usable = key_at < limit
            if t == 0:
                usable = usable | (key_at == query_at)
            words = jnp.concatenate(
                [
                    jnp.right_shift(
                        jnp.broadcast_to(bit_ref[block, t, w : w + 1, :], (per_word, tile)), bit_at
                    )
                    & 1
                    for w in range(word_count)
                ],
                axis=0,
            )
            allowed = (words == 1) & usable
            for h in range(heads):
                cols = slice(h * tile, (h + 1) * tile)
                part = jnp.where(allowed, scores[i * tile : (i + 1) * tile, cols], -jnp.inf)
                s_ref[t * tile : (t + 1) * tile, cols] = part
                top = jnp.max(part.reshape(tile // 8, 8, tile), axis=0)
                peaks[h] = top if peaks[h] is None else jnp.maximum(peaks[h], top)
    peak = jnp.max(jnp.concatenate(peaks, axis=1), axis=0, keepdims=True)
    group = math.gcd(heads, 2)
    mixed = [None] * (heads // group)
    total = None
    for t in range(0, slot_count, per_dot):
        weights = jnp.exp(s_ref[t * tile : (t + per_dot) * tile, :] - peak)
        part = jnp.sum(weights.reshape(per_dot * tile // 8, 8, heads * tile), axis=0)
        total = part if total is None else total + part
        weights = weights.astype(BF16)
        for g in range(heads // group):
            values = jnp.concatenate(
                [
                    vt_ref[g * group * HD : (g + 1) * group * HD, pl.ds(starts[t + i], tile)]
                    for i in range(per_dot)
                ],
                axis=1,
            )
            add = dot(values, weights[:, g * group * tile : (g + 1) * group * tile])
            mixed[g] = add if mixed[g] is None else mixed[g] + add
    total = jnp.sum(total, axis=0, keepdims=True)
    pieces = []
    for h in range(heads):
        g, i = divmod(h, group)
        own = mixed[g][i * HD : (i + 1) * HD, i * tile : (i + 1) * tile]
        pieces.append(own / total[:, h * tile : (h + 1) * tile])
    out_ref[pl.ds(out_at, tile), :] = jnp.concatenate(pieces, axis=0).T.astype(BF16)


def attend(sub_id, live_counts, tile_keys, queries_t, tile_bits, keys, values_t, first, count):
    blocks_own, slot_count, _, tile = tile_bits.shape
    head_cols, here = queries_t.shape
    per_sub = here // tile
    heads = head_cols // HD
    scratch = jax.ShapeDtypeStruct((math.gcd(count, 2), slot_count * tile, heads * tile), F32)
    vmem = pl.BlockSpec(memory_space=pltpu.VMEM)
    smem = pl.BlockSpec(memory_space=pltpu.SMEM)
    out = jax.ShapeDtypeStruct((count * tile, head_cols), BF16)
    bits = jax.ShapeDtypeStruct((blocks_own, slot_count, 8, tile), jnp.int32)
    return pl.pallas_call(
        functools.partial(attend_body, first, per_sub, blocks_own),
        out_shape=out,
        in_specs=[smem] * 3 + [vmem] * 4,
        out_specs=vmem,
        scratch_shapes=[pltpu.VMEM(scratch.shape, F32)],
        compiler_params=pltpu.CompilerParams(
            vmem_limit_bytes=vmem_limit(scratch, keys, values_t, queries_t, bits, out)
        ),
        name="attend",
    )(sub_id, live_counts, tile_keys, queries_t, tile_bits, keys, values_t)


def feed_body(first_row, chunk, paired, chan_ref, *refs):
    count = 2 if paired else 1
    mixed = refs[:count]
    x_ref, wo_ref, gain_ref, shift_ref, in_ref, out_w_ref, send_ref, keep_ref = refs[count:]
    chan_at = chan_ref[0]
    width = x_ref.shape[1]
    here = mixed[0].shape[0]
    gain, shift = gain_ref[1:2, :], shift_ref[1:2, :]

    def step(j, carry):
        at = pl.ds(pl.multiple_of(j * chunk, chunk), chunk)
        after = x_ref[pl.ds(pl.multiple_of(first_row + j * chunk, chunk), chunk), :].astype(F32)
        for i in range(count):
            cols = mixed[i].shape[1]
            if paired:
                chan_of = chan_at if i == 0 else 1 - chan_at
                weight = wo_ref[pl.ds(pl.multiple_of(chan_of * cols, cols), cols), :]
            else:
                weight = wo_ref[...]
            after = after + dot(mixed[i][at, :], weight)
        normed = normalize_rows(after, gain, shift).astype(BF16)
        hidden = jax.nn.gelu(dot(normed, in_ref[...], NT)).astype(BF16)
        update = dot(hidden, out_w_ref[...])
        if paired:
            half = width // 2
            first = chan_at == 0
            send_ref[at, :] = jnp.where(first, update[:, half:], update[:, :half]).astype(BF16)
            both = after + update
            keep_ref[at, :] = jnp.where(first, both[:, :half], both[:, half:])
        else:
            send_ref[at, :] = update.astype(BF16)
            keep_ref[at, :] = after
        return carry

    lax.fori_loop(0, here // chunk, step, 0)


def feed(chan_id, mixed, own_x, out_weight, gains, shifts, ffn_in, ffn_out, first_row):
    paired = len(mixed) == 2
    here, width = mixed[0].shape[0], own_x.shape[1]
    cols = width // 2 if paired else width
    vmem = pl.BlockSpec(memory_space=pltpu.VMEM)
    smem = pl.BlockSpec(memory_space=pltpu.SMEM)
    outs = (jax.ShapeDtypeStruct((here, cols), BF16), jax.ShapeDtypeStruct((here, cols), F32))
    return pl.pallas_call(
        functools.partial(feed_body, first_row, math.gcd(here, 256), paired),
        out_shape=outs,
        in_specs=[smem] + [vmem] * (len(mixed) + 6),
        out_specs=(vmem, vmem),
        compiler_params=pltpu.CompilerParams(
            vmem_limit_bytes=vmem_limit(*mixed, *outs, own_x, out_weight, ffn_in, ffn_out)
        ),
        name="feed",
    )(chan_id, *mixed, own_x, out_weight, gains, shifts, ffn_in, ffn_out)


def swap(array, axis):
    return lax.ppermute(array, axis, [(0, 1), (1, 0)])


def on_device(
    node_state,
    norm_gains,
    norm_shifts,
    query_weight,
    key_weight,
    value_weight,
    out_weight,
    ffn_in,
    ffn_out,
    live_counts,
    send_rows,
    tile_keys,
    tile_bits,
):
    n_chan = lax.axis_size("chan")
    n_sub = lax.axis_size("sub")
    n_space = lax.axis_size("space")
    paired = n_chan == 2 and n_sub == 2
    chan_at = lax.axis_index("chan")
    sub_at = lax.axis_index("sub")
    node_count, local_cols = node_state.shape
    tile = tile_bits.shape[-1]
    here = node_count // n_sub
    place = (chan_at.astype(jnp.int32).reshape(1), sub_at.astype(jnp.int32).reshape(1))
    up = [(i, i + 1) for i in range(n_space - 1)]
    down = [(i + 1, i) for i in range(n_space - 1)]

    if paired:
        across = swap(node_state, "chan")
        mains = [node_state, swap(node_state, "sub"), across, swap(across, "sub")]
    else:
        mains = [lax.all_gather(node_state, ("chan", "sub"), axis=1, tiled=True)]
    upward, downward = pick_rows(send_rows[0], node_state)
    lower = lax.ppermute(upward, "space", up)
    upper = lax.ppermute(downward, "space", down)
    halo = jnp.concatenate([lower, upper], axis=0)
    if paired:
        halo_across = swap(halo, "chan")
        halo_beside = swap(halo, "sub")
        halo_diagonal = swap(halo_across, "sub")
        halos = [halo, halo_beside, halo_across, halo_diagonal]
    else:
        halos = [lax.all_gather(halo, ("chan", "sub"), axis=1, tiled=True)]
    queries_w, values_w = flip(query_weight, value_weight)
    queries_t, keys, values_t, own_x = project(
        place, mains, norm_gains, norm_shifts, queries_w, key_weight, values_w, here
    )
    keys, values_t = extend(
        place, halos, norm_gains, norm_shifts, key_weight, values_w, keys, values_t
    )
    blocks_here = here // tile
    parts = math.gcd(blocks_here, 2)
    count = blocks_here // parts
    attended = []
    for i in range(parts):
        attended.append(
            attend(
                place[1], live_counts, tile_keys, queries_t, tile_bits, keys, values_t,
                i * count, count,
            )
        )
    finals = []
    for i in range(parts):
        if paired:
            mixed = [attended[i], swap(attended[i], "chan")]
        else:
            mixed = [lax.all_gather(attended[i], "chan", axis=1, tiled=True)]
        first_row = i * count * tile
        send, keep = feed(
            place[0], mixed, own_x, out_weight, norm_gains, norm_shifts, ffn_in, ffn_out,
            first_row,
        )
        if paired:
            total = keep + swap(send, "chan").astype(F32)
        else:
            width = keep.shape[1] // n_chan
            kept = lax.dynamic_slice_in_dim(keep, chan_at * width, width, 1)
            added = lax.psum_scatter(send, "chan", scatter_dimension=1, tiled=True)
            total = kept + added.astype(F32)
        position = sub_at * here + first_row + jnp.arange(total.shape[0], dtype=jnp.int32)
        finals.append(jnp.where((position < live_counts[0])[:, None], total, 0.0).astype(BF16))
    if paired:
        first = sub_at == 0
        mine, theirs = [], []
        for result in finals:
            left, right = result[:, :local_cols], result[:, local_cols:]
            mine.append(jnp.where(first, left, right))
            theirs.append(swap(jnp.where(first, right, left), "sub"))
        low = [jnp.where(first, a, b) for a, b in zip(mine, theirs)]
        high = [jnp.where(first, b, a) for a, b in zip(mine, theirs)]
        return jnp.concatenate(low + high, axis=0)
    result = jnp.concatenate(finals, axis=0)
    return lax.all_to_all(result, "sub", split_axis=1, concat_axis=0, tiled=True)


def solution(mesh):
    in_specs = (
        P(("ens", "space"), ("chan", "sub")),
        P(),
        P(),
        P(None, "chan"),
        P(None, "chan"),
        P(None, "chan"),
        P(),
        P("chan", None),
        P("chan", None),
        P("space"),
        P("space", None, None),
        P("space", None),
        P("space", None, None, None),
    )
    out_specs = P(("ens", "space"), ("chan", "sub"))

    return jax.shard_map(
        on_device, mesh=mesh, in_specs=in_specs, out_specs=out_specs, check_vma=False
    )
```
